32 devices in a mesh: ha: 4 (over y, x), wa: 8 (over z, core).
Axes of the slice: x: 2, y: 2, z: 4, core: 2. Of those that a mesh axis runs over, the one named last changes fastest.
Arguments:
- tokens: bfloat16 [112, 224, 384], P('ha', 'wa'), may hold values from -8 to 8
- cotangent: bfloat16 [112, 224, 384], P('ha', 'wa'), may hold values from -8 to 8
- w_qkv: bfloat16 [384, 1152], replicated, may hold values from -0.3125 to 0.3125
- w_proj: bfloat16 [384, 384], replicated, may hold values from -0.3125 to 0.3125
- w_fc1: bfloat16 [384, 1536], replicated, may hold values from -0.3125 to 0.3125
- w_fc2: bfloat16 [1536, 384], replicated, may hold values from -0.15625 to 0.15625
- bias_table: float32 [169, 12], replicated, may hold values from -4 to 280
- rel_index: int32 [49, 49], replicated, may hold values from 0 to 168, as said below
- region: int32 [112, 224], P('ha', 'wa'), may hold values from 0 to 15, as said below
Outputs:
- block_out: bfloat16 [112, 224, 384], P('ha', 'wa')
- token_grad: bfloat16 [112, 224, 384], P('ha', 'wa')
- grad_qkv: float32 [384, 1152], replicated
- grad_proj: float32 [384, 384], replicated
- grad_fc1: float32 [384, 1536], replicated
- grad_fc2: float32 [1536, 384], replicated
- grad_table: float32 [169, 12], replicated
The draws below stay inside these ranges and needn't reach their ends.
Inputs may be any that keep to these rules, and one draw needn't show every extreme that they name: `rel_index`: pairs of window positions with the same offset share an entry, pairs with different offsets have different entries. `region`: the crop id of the token at each position of the shifted grid.
All inputs are finite; a program needn't handle non-finite values.
Results may differ from the reference program's by a relative error of at most 0.016.
Values may be sent and summed in bfloat16 or wider, within the bound.
A program may use at most 128 MiB of HBM per device.

```python
import math
import jax
import jax.numpy as jnp
from jax import lax

C = 384
HEADS = 12
FFN = 1536
SIDE = 7
SHIFT = 3
CROPS = 4
HEAD_DIM = 32
WINDOW = 49
TABLE = 169
NH = 112
NW = 224
PARAMS = 1771500


def field_drawn(key, salt):
    values = jax.random.normal(jax.random.fold_in(key, salt), (NH, NW, C), jnp.float32)
    return jnp.clip(values, -8.0, 8.0).astype(jnp.bfloat16)


def draw_tokens(key, part):
    return field_drawn(key, 31)


def draw_cotangent(key, part):
    return field_drawn(key, 41)


def label_order(key):
    return jax.random.permutation(jax.random.fold_in(key, 7), TABLE).astype(jnp.int32)


def draw_rel_index(key, part):
    order = label_order(key)
    places = jnp.arange(WINDOW, dtype=jnp.int32)
    offset_rows = places[:, None] // SIDE - places[None, :] // SIDE + SIDE - 1
    offset_cols = places[:, None] % SIDE - places[None, :] % SIDE + SIDE - 1
    return order[offset_rows * (2 * SIDE - 1) + offset_cols]


def draw_bias_table(key, part):
    values = jax.random.normal(jax.random.fold_in(key, 21), (TABLE, HEADS), jnp.float32)
    return jnp.clip(values, -4.0, 4.0)


def crop_of(places, cuts):
    return jnp.sum((places[:, None] >= cuts[None, :]).astype(jnp.int32), 1)


def draw_region(key, part):
    row_cuts = jax.random.randint(jax.random.fold_in(key, 3), (CROPS - 1,), 1, NH, dtype=jnp.int32)
    col_cuts = jax.random.randint(jax.random.fold_in(key, 4), (CROPS - 1,), 1, NW, dtype=jnp.int32)
    row_places = (jnp.arange(NH, dtype=jnp.int32) + SHIFT) % NH
    col_places = (jnp.arange(NW, dtype=jnp.int32) + SHIFT) % NW
    return crop_of(row_places, row_cuts)[:, None] * CROPS + crop_of(col_places, col_cuts)[None, :]


def scatter_about(own_key, shape, deviation, bound, held_as=jnp.bfloat16):
    return jnp.clip(deviation * jax.random.normal(own_key, shape, jnp.float32), -bound, bound).astype(held_as)


def setup_inputs(seed: int = 0) -> dict:
    splits = jax.random.split(jax.random.key(seed), 10)
    return {
        "tokens": draw_tokens(jax.random.fold_in(splits[9], 71), 0),
        "cotangent": draw_cotangent(jax.random.fold_in(splits[9], 71), 0),
        "w_qkv": scatter_about(splits[2], (C, 3 * C), C ** -0.5, 0.3125),
        "w_proj": scatter_about(splits[3], (C, C), C ** -0.5, 0.3125),
        "w_fc1": scatter_about(splits[4], (C, FFN), C ** -0.5, 0.3125),
        "w_fc2": scatter_about(splits[5], (FFN, C), FFN ** -0.5, 0.15625),
        "bias_table": draw_bias_table(jax.random.fold_in(splits[9], 71), 0),
        "rel_index": draw_rel_index(jax.random.fold_in(splits[9], 71), 0),
        "region": draw_region(jax.random.fold_in(splits[9], 71), 0),
    }


epsilon = 1e-05
highest = lax.Precision.HIGHEST

def rounded(values):
    return lax.optimization_barrier(values.astype(jnp.bfloat16)).astype(jnp.float32)

def normalize(values):
    average = lax.optimization_barrier(jnp.mean(values, -1, keepdims=True))
    centred = values - average
    inverse = lax.rsqrt(lax.optimization_barrier(jnp.mean(centred * centred, -1, keepdims=True)) + epsilon)
    return (centred * inverse, inverse)

def normalize_back(normal_rows, inverse, upstream):
    up_mean = lax.optimization_barrier(jnp.mean(upstream, -1, keepdims=True))
    cross_mean = lax.optimization_barrier(jnp.mean(upstream * normal_rows, -1, keepdims=True))
    return inverse * (upstream - up_mean - normal_rows * cross_mean)

def gelu_slope(pre_act):
    normal_cdf = 0.5 * (1.0 + lax.erf(pre_act * 2.0 ** (-0.5)))
    return normal_cdf + pre_act * jnp.exp(-0.5 * pre_act * pre_act) * (2.0 * math.pi) ** (-0.5)

def to_windows(grid_in):
    row_count, col_count = (grid_in.shape[0], grid_in.shape[1])
    shaped = grid_in.reshape(row_count // SIDE, SIDE, col_count // SIDE, SIDE, -1)
    return shaped.transpose(0, 2, 1, 3, 4).reshape(row_count // SIDE, col_count // SIDE, WINDOW, -1)

def from_windows(grid_in):
    band_count, across, channels = (grid_in.shape[0], grid_in.shape[1], grid_in.shape[3])
    shaped = grid_in.reshape(band_count, across, SIDE, SIDE, channels)
    return shaped.transpose(0, 2, 1, 3, 4).reshape(band_count * SIDE, across * SIDE, channels)

def attend(qkv_win, region_win, pos_bias):
    win_count = qkv_win.shape[0]
    parts_qkv = qkv_win.reshape(win_count, WINDOW, 3, HEADS, HEAD_DIM).astype(jnp.float32)
    queries, keys_in, values = (parts_qkv[:, :, 0], parts_qkv[:, :, 1], parts_qkv[:, :, 2])
    scores = jnp.einsum('wihd,wjhd->whij', queries, keys_in, precision=highest) * HEAD_DIM ** (-0.5) + pos_bias[None]
    same_region = region_win[:, :, None] == region_win[:, None, :]
    scores = jnp.where(same_region[:, None], scores, -1e+30)
    exponent = jnp.exp(scores - lax.optimization_barrier(jnp.max(scores, -1, keepdims=True)))
    attn_probs = exponent / lax.optimization_barrier(jnp.sum(exponent, -1, keepdims=True))
    weighted = jnp.einsum('whij,wjhd->wihd', rounded(attn_probs), values, precision=highest)
    return (weighted.reshape(win_count, WINDOW, HEADS * HEAD_DIM).astype(jnp.bfloat16), attn_probs)

def attend_back(qkv_win, attn_probs, upstream):
    win_count = qkv_win.shape[0]
    parts_qkv = qkv_win.reshape(win_count, WINDOW, 3, HEADS, HEAD_DIM).astype(jnp.float32)
    queries, keys_in, values = (parts_qkv[:, :, 0], parts_qkv[:, :, 1], parts_qkv[:, :, 2])
    grad_out = upstream.reshape(win_count, WINDOW, HEADS, HEAD_DIM).astype(jnp.float32)
    grad_probs = jnp.einsum('wihd,wjhd->whij', grad_out, values, precision=highest)
    grad_values = jnp.einsum('whij,wihd->wjhd', rounded(attn_probs), grad_out, precision=highest)
    grad_scores = attn_probs * (grad_probs - lax.optimization_barrier(jnp.sum(attn_probs * grad_probs, -1, keepdims=True)))
    bias_grad = lax.optimization_barrier(jnp.sum(grad_scores, 0))
    scaled = rounded(grad_scores * HEAD_DIM ** (-0.5))
    grad_queries = jnp.einsum('whij,wjhd->wihd', scaled, keys_in, precision=highest)
    grad_keys = jnp.einsum('whij,wihd->wjhd', scaled, queries, precision=highest)
    stacked = jnp.stack([grad_queries, grad_keys, grad_values], 2)
    return (stacked.reshape(win_count, WINDOW, 3 * HEADS * HEAD_DIM).astype(jnp.bfloat16), bias_grad)

def reference(tokens, cotangent, w_qkv, w_proj, w_fc1, w_fc2, bias_table, rel_index, region):
    row_count, col_count, channels = tokens.shape
    lookup = (rel_index.reshape(-1)[:, None] == jnp.arange(TABLE, dtype=jnp.int32)[None, :]).astype(jnp.float32)
    pos_bias = jnp.dot(lookup, bias_table, precision=highest).T.reshape(HEADS, WINDOW, WINDOW)
    token_f32 = tokens.astype(jnp.float32)
    first_norm, first_scale = normalize(token_f32)
    shifted = jnp.roll(first_norm.astype(jnp.bfloat16), (-SHIFT, -SHIFT), (0, 1))
    flat_shift = shifted.reshape(-1, channels)
    qkv_tok = jnp.dot(flat_shift, w_qkv, preferred_element_type=jnp.float32).astype(jnp.bfloat16)
    qkv_win = to_windows(qkv_tok.reshape(row_count, col_count, 3 * channels))
    region_win = to_windows(region[..., None])[..., 0]

    def forward_band(operands):
        return attend(operands[0], operands[1], pos_bias)
    attn_win, attn_probs = lax.map(forward_band, (qkv_win, region_win))
    attn_tok = from_windows(attn_win).reshape(-1, channels)
    projected = jnp.dot(attn_tok, w_proj, preferred_element_type=jnp.float32).astype(jnp.bfloat16)
    middle = token_f32 + jnp.roll(projected.reshape(row_count, col_count, channels), (SHIFT, SHIFT), (0, 1)).astype(jnp.float32)
    second_norm, second_scale = normalize(middle)
    normed_low = second_norm.astype(jnp.bfloat16).reshape(-1, channels)
    pre_act = jnp.dot(normed_low, w_fc1, preferred_element_type=jnp.float32)
    activated = jax.nn.gelu(pre_act, approximate=False).astype(jnp.bfloat16)
    block_out = (middle + jnp.dot(activated, w_fc2, preferred_element_type=jnp.float32).reshape(row_count, col_count, channels)).astype(jnp.bfloat16)
    upstream = cotangent.reshape(-1, channels)
    raw_fc2 = jnp.dot(activated.T, upstream, preferred_element_type=jnp.float32)
    grad_pre = (jnp.dot(upstream, w_fc2.T, preferred_element_type=jnp.float32) * gelu_slope(pre_act)).astype(jnp.bfloat16)
    raw_fc1 = jnp.dot(normed_low.T, grad_pre, preferred_element_type=jnp.float32)
    grad_second = jnp.dot(grad_pre, w_fc1.T, preferred_element_type=jnp.float32).reshape(row_count, col_count, channels)
    grad_mid = cotangent.astype(jnp.float32) + normalize_back(second_norm, second_scale, grad_second)
    back_rolled = jnp.roll(grad_mid.astype(jnp.bfloat16), (-SHIFT, -SHIFT), (0, 1)).reshape(-1, channels)
    raw_proj = jnp.dot(attn_tok.T, back_rolled, preferred_element_type=jnp.float32)
    grad_attn = jnp.dot(back_rolled, w_proj.T, preferred_element_type=jnp.float32).astype(jnp.bfloat16)
    attn_back = to_windows(grad_attn.reshape(row_count, col_count, channels))

    def backward_band(operands):
        return attend_back(operands[0], operands[1], operands[2])
    qkv_grads, bias_parts = lax.map(backward_band, (qkv_win, attn_probs, attn_back))
    bias_grad = lax.optimization_barrier(jnp.sum(bias_parts, 0))
    raw_table = jnp.dot(lookup.T, bias_grad.reshape(HEADS, -1).T, precision=highest)
    qkv_back = from_windows(qkv_grads).reshape(-1, 3 * channels)
    raw_qkv = jnp.dot(flat_shift.T, qkv_back, preferred_element_type=jnp.float32)
    grad_shift = jnp.dot(qkv_back, w_qkv.T, preferred_element_type=jnp.float32).astype(jnp.bfloat16)
    grad_normed = jnp.roll(grad_shift.reshape(row_count, col_count, channels), (SHIFT, SHIFT), (0, 1))
    token_grad = (grad_mid + normalize_back(first_norm, first_scale, grad_normed.astype(jnp.float32))).astype(jnp.bfloat16)
    raw = (raw_qkv, raw_proj, raw_fc1, raw_fc2, raw_table)
    norm_sq = jnp.sum(jnp.stack([jnp.sum(gradient * gradient) for gradient in raw]))
    factor = jnp.minimum(1.0, math.sqrt(PARAMS) / (jnp.sqrt(norm_sq) + 1e-06))
    return (block_out, token_grad, raw_qkv * factor, raw_proj * factor, raw_fc1 * factor, raw_fc2 * factor, raw_table * factor)
```

```python
import functools
import math

import jax
import jax.numpy as jnp
from jax import lax
from jax.experimental import pallas as pl
from jax.experimental.pallas import tpu as pltpu
from jax.sharding import PartitionSpec as P

HEADS = 12
SIDE = 7
SHIFT = 3
HEAD_DIM = 32
TABLE = 169
PARAMS = 1771500
CELL = 8
SLOTS = CELL * CELL
GROUP = 4
LANES = GROUP * HEAD_DIM
GROUPS = HEADS // GROUP
FFN_CHUNKS = 3

epsilon = 1e-05
highest = lax.Precision.HIGHEST
f32 = jnp.float32
bf16 = jnp.bfloat16


def from_behind(x, axis, by):
    count = lax.axis_size(axis)
    return lax.ppermute(x, axis, [(i, (i + by) % count) for i in range(count)])


def to_shifted(grid_in):
    lower_rim = from_behind(grid_in[:SHIFT], "ha", -1)
    taller = jnp.concatenate([grid_in[SHIFT:], lower_rim], 0)
    right_rim = from_behind(taller[:, :SHIFT], "wa", -1)
    return jnp.concatenate([taller[:, SHIFT:], right_rim], 1)


def from_shifted(grid_in):
    upper_rim = from_behind(grid_in[-SHIFT:], "ha", 1)
    taller = jnp.concatenate([upper_rim, grid_in[:-SHIFT]], 0)
    left_rim = from_behind(taller[:, -SHIFT:], "wa", 1)
    return jnp.concatenate([left_rim, taller[:, :-SHIFT]], 1)


def to_cells(grid_in, fill):
    rows, cols, channels = grid_in.shape
    split = grid_in.reshape(rows // SIDE, SIDE, cols // SIDE, SIDE, channels)
    extra = CELL - SIDE
    padded = jnp.pad(
        split, ((0, 0), (0, extra), (0, 0), (0, extra), (0, 0)), constant_values=fill
    )
    return padded.transpose(0, 2, 1, 3, 4).reshape(-1, channels)


def from_cells(flat, rows, cols):
    split = flat.reshape(rows // SIDE, cols // SIDE, CELL, CELL, -1)[:, :, :SIDE, :SIDE]
    return split.transpose(0, 2, 1, 3, 4).reshape(rows, cols, -1)


def normalize(values):
    average = jnp.mean(values, -1, keepdims=True)
    centred = values - average
    inverse = lax.rsqrt(jnp.mean(centred * centred, -1, keepdims=True) + epsilon)
    return (centred * inverse, inverse)


def normalize_back(normal_rows, inverse, upstream):
    up_mean = jnp.mean(upstream, -1, keepdims=True)
    cross_mean = jnp.mean(upstream * normal_rows, -1, keepdims=True)
    return inverse * (upstream - up_mean - normal_rows * cross_mean)


def product(left, right, left_dim, right_dim):
    return lax.dot_general(
        left, right, (((left_dim,), (right_dim,)), ((), ())), preferred_element_type=f32
    )


def head_mask():
    shape = (GROUP * SLOTS, LANES)
    row_head = lax.broadcasted_iota(jnp.int32, shape, 0) // SLOTS
    lane_head = lax.broadcasted_iota(jnp.int32, shape, 1) // HEAD_DIM
    return (row_head == lane_head).astype(f32)


def stack_heads(rows, mask):
    return jnp.concatenate([rows] * GROUP, 0) * mask


def gather_heads(stacked, mask):
    kept = stacked * mask
    total = kept[:SLOTS]
    for head in range(1, GROUP):
        total = total + kept[head * SLOTS : (head + 1) * SLOTS]
    return total


def forward_kernel(
    windows, steps, tok_ref, ct_ref, col_ref, row_ref, bias_ref, wq_ref, wp_ref, w1_ref, w2_ref,
    out_ref, mid_ref, qkv_ref, attn_ref, probs_ref, g1_ref, g2_ref, acc1, acc2,
):
    step = pl.program_id(0)

    @pl.when(step == 0)
    def _():
        acc1[...] = jnp.zeros_like(acc1)
        acc2[...] = jnp.zeros_like(acc2)

    channels = tok_ref.shape[1]
    token = tok_ref[...].astype(f32)
    normal, _ = normalize(token)
    qkv_ref[...] = product(normal.astype(bf16), wq_ref[...], 1, 0).astype(bf16)
    mask = head_mask()
    mask_low = mask.astype(bf16)
    for w in range(windows):
        at = slice(w * SLOTS, (w + 1) * SLOTS)
        same = col_ref[at, :] == row_ref[w]
        hidden = jnp.where(same, 0.0, -1e30)
        hidden = jnp.concatenate([hidden] * GROUP, 0)
        for g in range(GROUPS):
            lanes = g * LANES
            query = stack_heads(qkv_ref[at, lanes : lanes + LANES], mask_low)
            key = qkv_ref[at, channels + lanes : channels + lanes + LANES]
            value = qkv_ref[at, 2 * channels + lanes : 2 * channels + lanes + LANES]
            bias = bias_ref[g * GROUP * SLOTS : (g + 1) * GROUP * SLOTS, :]
            scores = product(query, key, 1, 1) * HEAD_DIM ** (-0.5) + bias + hidden
            exponent = jnp.exp(scores - jnp.max(scores, -1, keepdims=True))
            probs = exponent * (1.0 / jnp.sum(exponent, -1, keepdims=True))
            start = (w * GROUPS + g) * GROUP * SLOTS
            probs_ref[start : start + GROUP * SLOTS, :] = probs
            mixed = product(probs.astype(bf16), value, 1, 0)
            attn_ref[at, lanes : lanes + LANES] = gather_heads(mixed, mask).astype(bf16)
    projected = product(attn_ref[...], wp_ref[...], 1, 0).astype(bf16)
    middle = token + projected.astype(f32)
    second, scale = normalize(middle)
    low = second.astype(bf16)
    upstream = ct_ref[...]
    low_turned = low.T
    up_turned = upstream.T
    hidden_units = w1_ref.shape[1]
    width = hidden_units // FFN_CHUNKS
    total = middle
    back = jnp.zeros_like(middle)
    for c in range(FFN_CHUNKS):
        at = slice(c * width, (c + 1) * width)
        w1 = w1_ref[:, at]
        w2 = w2_ref[at, :]
        pre = product(low, w1, 1, 0)
        cdf = 0.5 * (1.0 + lax.erf(pre * 2.0 ** (-0.5)))
        density = jnp.exp(-0.5 * pre * pre) * (2.0 * math.pi) ** (-0.5)
        active = (pre * cdf).astype(bf16)
        total = total + product(active, w2, 1, 0)
        acc2[:, at] += product(up_turned, active, 1, 0)
        grad_pre = (product(upstream, w2, 1, 1) * (cdf + pre * density)).astype(bf16)
        acc1[:, at] += product(low_turned, grad_pre, 1, 0)
        back = back + product(grad_pre, w1, 1, 1)
    out_ref[...] = total.astype(bf16)
    mid_ref[...] = upstream.astype(f32) + normalize_back(second, scale, back)

    @pl.when(step == steps - 1)
    def _():
        g1_ref[...] = acc1[...].astype(bf16)
        g2_ref[...] = acc2[...].T.astype(bf16)


def backward_kernel(
    windows, steps, tok_ref, mid_ref, qkv_ref, attn_ref, probs_ref, wq_ref, wp_ref,
    grad_ref, packed_ref, table_ref, accq, accp, up_ref, gq_ref,
):
    step = pl.program_id(0)

    @pl.when(step == 0)
    def _():
        accq[...] = jnp.zeros_like(accq)
        accp[...] = jnp.zeros_like(accp)
        table_ref[...] = jnp.zeros_like(table_ref)

    channels = tok_ref.shape[1]
    grad_mid = mid_ref[...]
    low = grad_mid.astype(bf16)
    accp[...] += product(attn_ref[...], low, 0, 0)
    up_ref[...] = product(low, wp_ref[...], 1, 1).astype(bf16)
    mask = head_mask()
    mask_low = mask.astype(bf16)
    for w in range(windows):
        at = slice(w * SLOTS, (w + 1) * SLOTS)
        for g in range(GROUPS):
            first = slice(g * LANES, (g + 1) * LANES)
            second = slice(channels + g * LANES, channels + (g + 1) * LANES)
            third = slice(2 * channels + g * LANES, 2 * channels + (g + 1) * LANES)
            rows = slice(g * GROUP * SLOTS, (g + 1) * GROUP * SLOTS)
            query = stack_heads(qkv_ref[at, first], mask_low)
            key = qkv_ref[at, second]
            value = qkv_ref[at, third]
            upstream = stack_heads(up_ref[at, first], mask_low)
            start = (w * GROUPS + g) * GROUP * SLOTS
            probs = probs_ref[start : start + GROUP * SLOTS, :]
            grad_probs = product(upstream, value, 1, 1)
            inner = jnp.sum(probs * grad_probs, -1, keepdims=True)
            grad_scores = probs * (grad_probs - inner)
            table_ref[rows, :] += grad_scores
            scaled = (grad_scores * HEAD_DIM ** (-0.5)).astype(bf16)
            gq_ref[at, first] = gather_heads(product(scaled, key, 1, 0), mask).astype(bf16)
            gq_ref[at, second] = product(scaled, query, 0, 0).astype(bf16)
            gq_ref[at, third] = product(probs.astype(bf16), upstream, 0, 0).astype(bf16)
    normal, scale = normalize(tok_ref[...].astype(f32))
    grads = gq_ref[...]
    accq[...] += product(normal.astype(bf16), grads, 0, 0)
    grad_normed = product(grads, wq_ref[...], 1, 1).astype(bf16).astype(f32)
    grad_ref[...] = (grad_mid + normalize_back(normal, scale, grad_normed)).astype(bf16)

    @pl.when(step == steps - 1)
    def _():
        packed_ref[...] = jnp.zeros_like(packed_ref)
        packed_ref[:channels, : 3 * channels] = accq[...].astype(bf16)
        packed_ref[:channels, 3 * channels :] = accp[...].astype(bf16)


def rows_of(shape, at=0):
    return pl.BlockSpec(shape, lambda i: (i, at))


def whole(shape):
    return pl.BlockSpec(shape, lambda i: (0,) * len(shape))


def local(tokens, cotangent, w_qkv, w_proj, w_fc1, w_fc2, bias_table, rel_index, region):
    tile_rows, tile_cols, channels = tokens.shape
    ffn = w_fc1.shape[1]
    count = (tile_rows // SIDE) * (tile_cols // SIDE)
    windows = math.gcd(count, 4)
    steps = count // windows
    block = windows * SLOTS
    total = count * SLOTS

    both = to_shifted(jnp.concatenate([tokens, cotangent], -1))
    cells = to_cells(both, 0)
    region_cells = to_cells(region[..., None], -1)
    region_rows = region_cells.reshape(count, 1, SLOTS)

    extra = CELL - SIDE
    places = jnp.pad(
        rel_index.reshape(SIDE, SIDE, SIDE, SIDE), ((0, extra),) * 4, constant_values=-1
    ).reshape(1, SLOTS * SLOTS)
    lookup = (jnp.arange(TABLE, dtype=jnp.int32)[:, None] == places).astype(f32)
    pos_bias = lax.dot_general(
        bias_table, lookup, (((0,), (0,)), ((), ())), precision=highest
    ).reshape(HEADS * SLOTS, SLOTS)

    params = pltpu.CompilerParams(
        dimension_semantics=("arbitrary",), vmem_limit_bytes=60 * 1024 * 1024
    )
    shape = jax.ShapeDtypeStruct
    block_cells, grad_mid, qkv, attn, probs, grad_fc1, grad_fc2 = pl.pallas_call(
        functools.partial(forward_kernel, windows, steps),
        name="forward",
        grid=(steps,),
        in_specs=[
            rows_of((block, channels)),
            rows_of((block, channels), 1),
            rows_of((block, 1)),
            pl.BlockSpec((windows, 1, SLOTS), lambda i: (i, 0, 0)),
            whole((HEADS * SLOTS, SLOTS)),
            whole((channels, 3 * channels)),
            whole((channels, channels)),
            whole((channels, ffn)),
            whole((ffn, channels)),
        ],
        out_specs=[
            rows_of((block, channels)),
            rows_of((block, channels)),
            rows_of((block, 3 * channels)),
            rows_of((block, channels)),
            rows_of((windows * HEADS * SLOTS, SLOTS)),
            whole((channels, ffn)),
            whole((ffn, channels)),
        ],
        out_shape=[
            shape((total, channels), bf16),
            shape((total, channels), f32),
            shape((total, 3 * channels), bf16),
            shape((total, channels), bf16),
            shape((count * HEADS * SLOTS, SLOTS), f32),
            shape((channels, ffn), bf16),
            shape((ffn, channels), bf16),
        ],
        scratch_shapes=[pltpu.VMEM((channels, ffn), f32), pltpu.VMEM((channels, ffn), f32)],
        compiler_params=params,
        cost_estimate=pl.CostEstimate(
            flops=20_000_000_000, bytes_accessed=20_000_000, transcendentals=4_000_000
        ),
    )(cells, cells, region_cells, region_rows, pos_bias, w_qkv, w_proj, w_fc1, w_fc2)
    summed_ffn = lax.psum((grad_fc1, grad_fc2), ("ha", "wa"))
    block_out = from_shifted(from_cells(block_cells, tile_rows, tile_cols))

    packed_rows = channels + 16
    grad_cells, packed, bias_grad = pl.pallas_call(
        functools.partial(backward_kernel, windows, steps),
        name="backward",
        grid=(steps,),
        in_specs=[
            rows_of((block, channels)),
            rows_of((block, channels)),
            rows_of((block, 3 * channels)),
            rows_of((block, channels)),
            rows_of((windows * HEADS * SLOTS, SLOTS)),
            whole((channels, 3 * channels)),
            whole((channels, channels)),
        ],
        out_specs=[
            rows_of((block, channels)),
            whole((packed_rows, 4 * channels)),
            whole((HEADS * SLOTS, SLOTS)),
        ],
        out_shape=[
            shape((total, channels), bf16),
            shape((packed_rows, 4 * channels), bf16),
            shape((HEADS * SLOTS, SLOTS), f32),
        ],
        scratch_shapes=[
            pltpu.VMEM((channels, 3 * channels), f32),
            pltpu.VMEM((channels, channels), f32),
            pltpu.VMEM((block, channels), bf16),
            pltpu.VMEM((block, 3 * channels), bf16),
        ],
        compiler_params=params,
        cost_estimate=pl.CostEstimate(
            flops=16_000_000_000, bytes_accessed=16_000_000, transcendentals=1_000_000
        ),
    )(cells, grad_mid, qkv, attn, probs, w_qkv, w_proj)
    grad_table = lax.dot_general(
        bias_grad.reshape(HEADS, SLOTS * SLOTS), lookup, (((1,), (1,)), ((), ())), precision=highest
    )
    packed = lax.dynamic_update_slice(packed, grad_table.astype(bf16), (channels, 0))
    packed, summed_ffn = lax.optimization_barrier((packed, summed_ffn))
    summed = lax.psum(packed, ("ha", "wa")).astype(f32)
    token_grad = from_shifted(from_cells(grad_cells, tile_rows, tile_cols))

    fc1 = summed_ffn[0].astype(f32)
    fc2 = summed_ffn[1].astype(f32)
    norm_sq = jnp.sum(fc1 * fc1) + jnp.sum(fc2 * fc2) + jnp.sum(summed * summed)
    factor = jnp.minimum(1.0, math.sqrt(PARAMS) / (jnp.sqrt(norm_sq) + 1e-06))
    return (
        block_out,
        token_grad,
        summed[:channels, : 3 * channels] * factor,
        summed[:channels, 3 * channels :] * factor,
        fc1 * factor,
        fc2 * factor,
        summed[channels : channels + HEADS, :TABLE].T * factor,
    )


def solution(mesh):
    placed = (P("ha", "wa", None), P("ha", "wa", None), P(), P(), P(), P(), P(), P(), P("ha", "wa"))
    return jax.shard_map(
        local,
        mesh=mesh,
        in_specs=placed,
        out_specs=(P("ha", "wa", None), P("ha", "wa", None), P(), P(), P(), P(), P()),
        check_vma=False,
    )
```
